512 devices in a mesh: group: 2 (over y), expert: 32 (over z), tensor: 4 (over x), sub: 2 (over core).
Axes of the slice: x: 4, y: 2, z: 32, core: 2. Of those that a mesh axis runs over, the one named last changes fastest.
The devices are a block of a 4x16x32 slice.
Arguments:
- tokens: bfloat16 [512, 7168], P(('group', 'expert', 'sub')), parts along dimension 0, may hold values from -6 to 6
- expert_ids: int32 [512, 8], P(('group', 'expert', 'sub')), parts along dimension 0, may hold values from 0 to 15, all different within a row; in each aligned block of 4 rows (0 to 3, 4 to 7, ...) at most 3 rows name the same one
- gate_codes: int32 [512, 8], P(('group', 'expert', 'sub')), parts along dimension 0, may hold values from 1 to 63
- w_gate: bfloat16 [32, 1024, 7168], P('expert', ('tensor', 'sub')), may hold values from -0.0625 to 0.0625
- w_up: bfloat16 [32, 1024, 7168], P('expert', ('tensor', 'sub')), may hold values from -0.0625 to 0.0625
- w_down: bfloat16 [32, 1024, 7168], P('expert', ('tensor', 'sub')), may hold values from -0.125 to 0.125
Outputs:
- mixed: bfloat16 [512, 7168], P(('group', 'expert', 'sub'), 'tensor'), parts along dimension 0
The draws below stay inside these ranges and needn't reach their ends.
There are 2 independent parts, one for each index of `group`. The reference program is written for one: setup_inputs(seed, part) draws one part's arguments, and reference() takes and returns one part's arrays. A program takes and returns all parts, laid end to end along the dimension named above; an argument that names none is the same for every part. Nothing has to cross between parts.
Inputs may be any that keep to these rules, and one draw needn't show every extreme that they name: `expert_ids`: the 8 numbers of a row differ; within the rows of one device (aligned blocks of 4 rows) no expert is named by more than 3 rows, a bound that some block reaches.
All inputs are finite; a program needn't handle non-finite values.
Results may differ from the reference program's by a relative error of at most 0.008.
Values may be sent and summed in bfloat16 or wider, within the bound.
A program may use at most 64 MiB of HBM per device.

```python
import math
import jax
import jax.numpy as jnp
import numpy as np
from jax import lax

D = 7168
FF = 2048
TOK_DEV = 4
EXPERTS = 16
HALVES = 32
TOP = 8
CAP = 3
RUN = 128
TOKENS = 256


def set_ends(drawn, rng, smallest, high):
    spot = [jax.random.randint(jax.random.fold_in(rng, axis), (), 0, length) for axis, length in enumerate(drawn.shape)]
    widest = drawn.shape.index(max(drawn.shape))
    next_to = spot[:widest] + [(spot[widest] + 1) % drawn.shape[widest]] + spot[widest + 1:]
    return drawn.at[tuple(spot)].set(smallest).at[tuple(next_to)].set(high)


def block_scale(key, extent, cuts, low, top_value):
    def one(position, parts):
        steps = jax.random.uniform(jax.random.fold_in(jax.random.fold_in(key, 6), position), (parts,), jnp.float32, low / len(cuts), top_value / len(cuts))
        return jnp.repeat(jnp.exp(steps), extent[position] // parts).reshape((-1,) + (1,) * (len(extent) - position - 1))

    factor_of = one(*cuts[0])
    for cut in cuts[1:]:
        factor_of = factor_of * one(*cut)
    return factor_of


def deal_out(key, own, number, rows, count, top, bound, lean):
    ranking = jax.random.permutation(key, count)
    heavy_load, usual = load_shares(count, rows * top, bound, lean, True), load_shares(count, rows * top, bound, lean, False)
    places = jnp.arange(count)

    def named(tallies, turn):
        used = int((tallies > 0).sum())
        fixed = max(1, used // 4)
        moved = fixed + (places - fixed + turn * (used - fixed)) % max(1, count - fixed)
        return jnp.zeros((count,), jnp.int32).at[ranking[jnp.where(places < fixed, places, moved)]].set(jnp.asarray(tallies, jnp.int32))

    tallies = jnp.where(number % 4 == 0, named(heavy_load, number // 4), named(usual, number - number // 4 - 1))
    mixed = jax.random.permutation(jax.random.fold_in(own, 3), count)
    giver, receiver = mixed[0:count // 2 * 2:2], mixed[1:count // 2 * 2:2]
    slack = jnp.minimum(tallies[giver] - 1, bound - tallies[receiver]) // 2
    slack = jnp.where((giver == ranking[0]) | (receiver == ranking[0]) | (tallies[receiver] == 0), 0, jnp.maximum(slack, 0))
    moved = jax.random.randint(jax.random.fold_in(own, 4), (count // 2,), 0, 1 << 20) % (slack + 1)
    tallies = tallies.at[giver].add(-moved).at[receiver].add(moved)
    items = jnp.searchsorted(jnp.cumsum(tallies), jnp.arange(rows * top), side="right").astype(jnp.int32)
    table = items.reshape(top, rows).T
    table = table[jax.random.permutation(jax.random.fold_in(own, 1), rows)]
    turn = jax.random.randint(jax.random.fold_in(own, 2), (rows, 1), 0, top)
    return jnp.take_along_axis(table, (jnp.arange(top)[None, :] + turn) % top, axis=1)


def load_shares(count, total, bound, skew, full):
    loads = [(1 << 20) // math.isqrt(rank ** skew) + 1 for rank in range(1, count + 1)]
    largest = bound if full else min(bound, max(-(-total // count), total * loads[0] // sum(loads)))
    least = 1 if total - largest >= count - 1 else 0
    counts, spare = [largest] + [least] * (count - 1), total - largest - least * (count - 1)
    while spare > 0:
        candidates = [i for i in range(1, count) if counts[i] < largest] or [i for i in range(1, count) if counts[i] < bound]
        pool, left = sum([loads[i] for i in candidates]), spare
        for i in candidates:
            more = min(bound - counts[i], max(1, left * loads[i] // pool), spare)
            counts[i] = counts[i] + more
            spare = spare - more
    return np.array(counts)


def normal_values(own_key, dims, deviation, most, pieces=(), held_as=jnp.bfloat16):
    gain = block_scale(own_key, dims, pieces, -0.22, 0.18) if pieces else 1.0
    drawn = jax.random.normal(own_key, dims, jnp.float32) * deviation * gain
    return jnp.minimum(jnp.maximum(drawn, -most), most).astype(held_as)


def setup_inputs(seed: int = 0, part: int = 0) -> dict:
    arg_keys = jax.random.split(jax.random.key(seed), 7)
    part_keys = jax.random.split(jax.random.fold_in(arg_keys[6], part), 7)
    tokens = normal_values(part_keys[0], (TOKENS, D), 1.0, 6.0, ((0, 64),))
    expert_ids_keys = jax.random.split(jax.random.fold_in(part_keys[1], 1), TOKENS // TOK_DEV)
    expert_ids_turns = jax.random.permutation(jax.random.fold_in(part_keys[1], 3), TOKENS // TOK_DEV)
    expert_ids = jax.vmap(lambda own, number: deal_out(jax.random.fold_in(part_keys[1], 2), own, number, TOK_DEV, EXPERTS, TOP, CAP, 1))(expert_ids_keys, expert_ids_turns).reshape((TOKENS, TOP))
    gate_codes = set_ends(jax.random.randint(part_keys[2], (TOKENS, TOP), 1, 64), jax.random.fold_in(part_keys[2], 1), 1, 63).astype(jnp.int32)
    w_gate = normal_values(arg_keys[3], (HALVES, FF // 2, D), D ** -0.5, 0.0625, ((0, 32), (1, 8)))
    w_up = normal_values(arg_keys[4], (HALVES, FF // 2, D), D ** -0.5, 0.0625, ((0, 32), (1, 8)))
    w_down = normal_values(arg_keys[5], (HALVES, FF // 2, D), FF ** -0.5, 0.125, ((0, 32), (1, 8)))
    return dict(tokens=tokens, expert_ids=expert_ids, gate_codes=gate_codes, w_gate=w_gate, w_up=w_up, w_down=w_down)


def reference(tokens, expert_ids, gate_codes, w_gate, w_up, w_down):
    weight = gate_codes.astype(jnp.float32) / 64.0
    token_count = tokens.shape[0]
    run_count = FF // RUN
    contract = (((1,), (1,)), ((), ()))

    def one_expert(total_out, expert):
        gate_full = jnp.concatenate([w_gate[2 * expert], w_gate[2 * expert + 1]], axis=0)
        up_full = jnp.concatenate([w_up[2 * expert], w_up[2 * expert + 1]], axis=0)
        down_full = jnp.concatenate([w_down[2 * expert], w_down[2 * expert + 1]], axis=0)
        gate_act = lax.dot_general(tokens, gate_full, contract, preferred_element_type=jnp.float32)
        up_act = lax.dot_general(tokens, up_full, contract, preferred_element_type=jnp.float32)
        hidden = (jax.nn.silu(gate_act) * up_act).astype(jnp.bfloat16)
        hid_runs = hidden.reshape(token_count, run_count, RUN).transpose(1, 0, 2)
        down_runs = down_full.reshape(run_count, RUN, D)

        def add_run(running, run_pair):
            hid_run, down_run = run_pair
            piece = jnp.dot(hid_run, down_run, preferred_element_type=jnp.float32).astype(jnp.bfloat16)
            piece = lax.optimization_barrier(piece)
            return running + piece.astype(jnp.float32), None

        summed, _ = lax.scan(add_run, jnp.zeros((token_count, D), jnp.float32), (hid_runs, down_runs))
        share_of = jnp.sum(jnp.where(expert_ids == expert, weight, jnp.float32(0.0)), axis=1)
        return total_out + share_of[:, None] * summed, None

    total_out, _ = lax.scan(one_expert, jnp.zeros((token_count, D), jnp.float32), jnp.arange(EXPERTS, dtype=jnp.int32))
    return total_out.astype(jnp.bfloat16)
```

```python
import functools

import jax
import jax.numpy as jnp
from jax import lax
from jax.experimental import pallas as pl
from jax.experimental.pallas import tpu as pltpu
from jax.sharding import PartitionSpec as P

MESH = pl.DeviceIdType.MESH
STRIDE = 4
LANES = 128
F32 = jnp.float32
BF16 = jnp.bfloat16


def plan(owners):
    last = owners // (2 * STRIDE)
    waves, rings = [], []
    for s in range(last + 1):
        d = STRIDE * s
        if s == 0:
            ring, near = [0], [1, -1, 2, -2]
        elif s < last:
            ring, near = [-d, d], [1 - d, 1 + d, -1 - d, -1 + d, -2 - d, 2 + d]
        else:
            ring, near = [d], [1 + d, -1 + d]
        rings.append(len(ring))
        waves.append([v % owners for v in ring + near])
    base = [0] + [v for s in range(1, last) for v in (-STRIDE * s, STRIDE * s)] + [STRIDE * last]
    order = base + [v + 1 for v in base] + [v - 1 for v in base]
    order += [2 + STRIDE * s for s in range(last)] + [-2 - STRIDE * s for s in range(last)]
    return waves, rings, base, [v % owners for v in order]


def kernel(
    owners, tensors, placed, w_gate, w_up, w_down, out,
    z_buf, partner_in, x_buf, c_buf, gu, dn, act, own, p_send, p_recv, s_buf, via, r_buf,
    near, far_send, far, fin, fin_recv,
    load, send, swap, ring_p, ring_m, local, x_in, x_fwd, c_in, pc, via_in, r_in, near_in, far_in, fin_in,
):
    waves, rings, base, order = plan(owners)
    last = len(waves) - 1
    flat = [v for wave in waves for v in wave]
    slot = {v: i for i, v in enumerate(flat)}
    starts = [sum(len(w) for w in waves[:s]) for s in range(last + 2)]
    place = {v: i for i, v in enumerate(order)}
    width = x_buf.shape[-1]
    rows = owners * z_buf.shape[1]
    runs = w_gate.shape[1]
    z, x, c = lax.axis_index("expert"), lax.axis_index("tensor"), lax.axis_index("sub")

    def at_z(d):
        return {"expert": lax.rem(z + (d % owners), owners)}

    def at_x(d):
        return {"tensor": lax.rem(x + (d % tensors), tensors)}

    partner = {"sub": 1 - c}

    def block_of(d, other):
        return lax.rem(x + (d % tensors), tensors) * 2 + (1 - c if other else c)

    loads = []
    for b in range(gu.shape[0]):
        cols = pl.ds(b * width, width)
        for src, dst in (
            (w_gate.at[0, :, cols], gu.at[b, 0:runs]),
            (w_up.at[0, :, cols], gu.at[b, runs : 2 * runs]),
            (w_down.at[0, :, cols], dn.at[b]),
        ):
            loads.append(pltpu.make_async_copy(src, dst, load.at[len(loads)]))
    for cp in loads:
        cp.start()

    peers = [at_z(d) for d in (STRIDE, -STRIDE, 1, -1, 2, -2)] + [at_x(1), at_x(-1), partner]
    barrier = pltpu.get_barrier_semaphore()
    for peer in peers:
        pl.semaphore_signal(barrier, inc=1, device_id=peer, device_id_type=MESH)
    pl.semaphore_wait(barrier, len(peers))

    sent = []

    def push(src, dst, sem, target):
        cp = pltpu.make_async_remote_copy(
            src_ref=src, dst_ref=dst, send_sem=send.at[len(sent)], recv_sem=sem,
            device_id=target, device_id_type=MESH,
        )
        cp.start()
        sent.append(cp)

    def arrive(ref, sem):
        pltpu.make_async_remote_copy(
            src_ref=ref, dst_ref=ref, send_sem=sem, recv_sem=sem,
            device_id=partner, device_id_type=MESH,
        ).wait_recv()

    push(placed.at[block_of(0, True)], partner_in, swap, partner)
    arrive(partner_in, swap)
    z_buf[0] = (placed[block_of(0, False)].astype(F32) + partner_in[...].astype(F32)).astype(BF16)

    def z_at(v):
        return z_buf.at[slot[v % owners]]

    def span(buf, s, lo=0, hi=None):
        hi = len(waves[s]) if hi is None else hi
        return buf.at[pl.ds(starts[s] + lo, hi - lo)]

    def z_part(s):
        return z_buf.at[pl.ds(starts[s], len(waves[s])), :, pl.ds(0, width)]

    def spread(v, up, down):
        push(z_at(v), z_at(v - 1), local.at[up], at_z(1))
        push(z_at(v), z_at(v + 1), local.at[up], at_z(-1))
        if down <= 0 and up < last:
            push(z_at(v), z_at(v - 2), local.at[up], at_z(2))
        if down >= 0 and up < last:
            push(z_at(v), z_at(v + 2), local.at[up], at_z(-2))

    def cut(s):
        n = len(waves[s])
        return n // 2 if s < last else n - n // 2

    def forward_x(s):
        arrive(span(x_buf.at[0], s), x_in.at[0, s])
        push(span(x_buf.at[0], s, 0, cut(s)), span(x_buf.at[2], s, 0, cut(s)), x_fwd.at[0, s], at_x(1))
        arrive(span(x_buf.at[1], s), x_in.at[1, s])
        push(span(x_buf.at[1], s, cut(s)), span(x_buf.at[2], s, cut(s)), x_fwd.at[1, s], at_x(-1))
        for i in (0, 1):
            push(span(x_buf.at[i], s), span(c_buf.at[1 + i], s), c_in.at[1 + i, s], partner)

    def finish_x(s):
        arrive(span(x_buf.at[2], s, 0, cut(s)), x_fwd.at[0, s])
        arrive(span(x_buf.at[2], s, cut(s)), x_fwd.at[1, s])
        push(span(x_buf.at[2], s), span(c_buf.at[3], s), c_in.at[3, s], partner)

    for s in range(last + 1):
        d = STRIDE * s
        if s > 0:
            arrive(z_at(-d), ring_p.at[s])
        if s < last:
            push(z_at(-d), z_at(-d - STRIDE), ring_p.at[s + 1], at_z(STRIDE))
        if 0 < s < last:
            arrive(z_at(d), ring_m.at[s])
        if s < last - 1:
            push(z_at(d), z_at(d + STRIDE), ring_m.at[s + 1], at_z(-STRIDE))
        if s == 0 or s == last:
            spread(d, s, 0)
        else:
            spread(-d, s, -1)
            spread(d, s, 1)
        arrive(span(z_buf, s, rings[s]), local.at[s])
        push(z_part(s), span(x_buf.at[0], s), x_in.at[0, s], at_x(1))
        push(z_part(s), span(x_buf.at[1], s), x_in.at[1, s], at_x(-1))
        push(z_part(s), span(c_buf.at[0], s), c_in.at[0, s], partner)
        if s >= 1:
            forward_x(s - 1)
        if s >= 2:
            finish_x(s - 2)

    for cp in loads:
        cp.wait()

    def multiply(ref, b, first=False):
        value = ref.astype(F32).reshape(rows, width).astype(BF16)
        part = lax.dot_general(value, gu[b], (((1,), (1,)), ((), ())), preferred_element_type=F32)
        act[...] = part if first else act[...] + part

    multiply(z_buf[:, :, 0:width], block_of(0, False), True)
    forward_x(last)
    finish_x(last - 1)
    multiply(x_buf[0], block_of(-1, False))
    multiply(x_buf[1], block_of(1, False))
    finish_x(last)
    for i, d in enumerate((0, -1, 1, 2)):
        for s in range(last + 1):
            arrive(span(c_buf.at[i], s), c_in.at[i, s])
        multiply(c_buf[i], block_of(d, True))
    multiply(x_buf[2], block_of(2, False))

    shares = z_buf[:, :, width:].astype(F32).reshape(rows, LANES)
    lane = lax.broadcasted_iota(jnp.int32, (rows, LANES), 1)
    share = jnp.sum(jnp.where(lane == z // 2, shares, 0.0), axis=1, keepdims=True)
    gate, up = act[:, 0:runs], act[:, runs:]
    hidden = (gate / (1.0 + jnp.exp(-gate)) * up * share).astype(BF16)

    def down(b):
        part = jnp.dot(hidden, dn[b], preferred_element_type=F32)
        return part.reshape(owners, rows // owners, width)

    steps = (2, 1, -1, 0)
    for i, d in enumerate(steps):
        part = down(block_of(d, True)).astype(BF16)
        for j, v in enumerate(flat):
            p_send[i, place[v]] = part[j]
        push(p_send.at[i], p_recv.at[i], pc.at[i], partner)
    for i, d in enumerate(steps):
        part = down(block_of(d, False))
        for j, v in enumerate(flat):
            own[i, place[v]] = part[j]

    half = owners // 2
    lo, hi = pl.ds(0, half), pl.ds(half, half)

    def both(i, part):
        return own[i, part] + p_recv[i, part].astype(F32)

    arrive(p_recv.at[0], pc.at[0])
    s_buf[0, lo] = both(0, lo).astype(BF16)
    push(s_buf.at[0, lo], via.at[0], via_in.at[0], at_x(1))
    s_buf[0, hi] = both(0, hi).astype(BF16)
    push(s_buf.at[0, hi], via.at[1], via_in.at[1], at_x(-1))
    arrive(p_recv.at[1], pc.at[1])
    s_buf[1, hi] = both(1, hi).astype(BF16)
    push(s_buf.at[1, hi], r_buf.at[0, hi], r_in.at[0, 1], at_x(1))
    arrive(p_recv.at[2], pc.at[2])
    s_buf[2, lo] = both(2, lo).astype(BF16)
    push(s_buf.at[2, lo], r_buf.at[1, lo], r_in.at[1, 0], at_x(-1))
    arrive(via.at[0], via_in.at[0])
    s_buf[1, lo] = (both(1, lo) + via[0].astype(F32)).astype(BF16)
    push(s_buf.at[1, lo], r_buf.at[0, lo], r_in.at[0, 0], at_x(1))
    arrive(via.at[1], via_in.at[1])
    s_buf[2, hi] = (both(2, hi) + via[1].astype(F32)).astype(BF16)
    push(s_buf.at[2, hi], r_buf.at[1, hi], r_in.at[1, 1], at_x(-1))
    arrive(p_recv.at[3], pc.at[3])
    for k in (0, 1):
        arrive(r_buf.at[0, lo if k == 0 else hi], r_in.at[0, k])
        arrive(r_buf.at[1, lo if k == 0 else hi], r_in.at[1, k])

    def summed(begin, size):
        part = pl.ds(begin, size)
        return both(3, part) + r_buf[0, part].astype(F32) + r_buf[1, part].astype(F32)

    count = len(base)
    begin = count
    for k, (size, d) in enumerate(((count, 1), (count, -1), (last, 2), (last, -2))):
        part = pl.ds(begin, size)
        s_buf[3, part] = summed(begin, size).astype(BF16)
        push(s_buf.at[3, part], near.at[pl.ds(begin - count, size)], near_in.at[k], at_z(d))
        begin += size
    begin = 0
    for k, size in enumerate((count, count, last, last)):
        arrive(near.at[pl.ds(begin, size)], near_in.at[k])
        begin += size

    def relayed(j):
        total = own[3, j] + p_recv[3, j].astype(F32) + r_buf[0, j].astype(F32) + r_buf[1, j].astype(F32)
        total = total + near[j].astype(F32) + near[count + j].astype(F32)
        for s in range(last):
            if base[j] == STRIDE * s:
                total = total + near[2 * count + s].astype(F32)
            if base[j] == -STRIDE * s:
                total = total + near[2 * count + last + s].astype(F32)
        return total

    for j in range(count - 1, 0, -1):
        far_send[j] = relayed(j).astype(BF16)
        push(far_send.at[j], far.at[j], far_in.at[j], at_z(base[j]))
    total = relayed(0)
    for j in range(1, count):
        arrive(far.at[j], far_in.at[j])
        total = total + far[j].astype(F32)
    fin[...] = total.astype(BF16)
    push(fin, fin_recv, fin_in, partner)
    out[c] = total.astype(BF16)
    arrive(fin_recv, fin_in)
    out[1 - c] = fin_recv[...]
    for cp in sent:
        cp.wait_send()


def shards(tokens, expert_ids, gate_codes, w_gate, w_up, w_down):
    tok_rows, features = tokens.shape
    owners, tensors, subs = lax.axis_size("expert"), lax.axis_size("tensor"), lax.axis_size("sub")
    blocks = tensors * subs
    width = features // blocks
    runs = w_gate.shape[1]
    chip_rows = tok_rows * subs
    waves, rings, base, order = plan(owners)
    last, count = len(waves) - 1, len(base)

    lane = jnp.arange(LANES, dtype=jnp.int32)
    share = jnp.where(expert_ids[:, :, None] == lane, gate_codes.astype(F32)[:, :, None] / 64.0, 0.0)
    share = jnp.sum(share, axis=1).astype(BF16)
    chunk = tokens.reshape(tok_rows, blocks, width).transpose(1, 0, 2)
    chunk = jnp.concatenate([chunk, jnp.broadcast_to(share, (blocks, tok_rows, LANES))], axis=2)
    mine = (jnp.arange(chip_rows) // tok_rows == lax.axis_index("sub"))[None, :, None]
    placed = jnp.where(mine, jnp.concatenate([chunk] * subs, axis=1), 0)

    def vmem(*shape, dtype=BF16):
        return pltpu.VMEM(shape, dtype)

    tile = (chip_rows, width)
    dma = pltpu.SemaphoreType.DMA
    whole = pl.BlockSpec(memory_space=pltpu.VMEM)
    away = pl.BlockSpec(memory_space=pl.ANY)
    mixed = pl.pallas_call(
        functools.partial(kernel, owners, tensors),
        out_shape=jax.ShapeDtypeStruct((subs,) + tile, BF16),
        in_specs=[whole, away, away, away],
        out_specs=whole,
        scratch_shapes=[
            vmem(owners, chip_rows, width + LANES),
            vmem(chip_rows, width + LANES),
            vmem(3, owners, *tile),
            vmem(4, owners, *tile),
            vmem(blocks, 2 * runs, width),
            vmem(blocks, runs, width),
            vmem(owners * chip_rows, 2 * runs, dtype=F32),
            vmem(4, owners, *tile, dtype=F32),
            vmem(4, owners, *tile),
            vmem(4, owners, *tile),
            vmem(4, owners, *tile),
            vmem(2, owners // 2, *tile),
            vmem(2, owners, *tile),
            vmem(owners - count, *tile),
            vmem(count, *tile),
            vmem(count, *tile),
            vmem(*tile),
            vmem(*tile),
            dma((3 * blocks,)),
            dma((112,)),
            dma,
            dma((last + 1,)),
            dma((last + 1,)),
            dma((last + 1,)),
            dma((2, last + 1)),
            dma((2, last + 1)),
            dma((4, last + 1)),
            dma((4,)),
            dma((2,)),
            dma((2, 2)),
            dma((4,)),
            dma((count,)),
            dma,
        ],
        compiler_params=pltpu.CompilerParams(
            collective_id=0, has_side_effects=True, vmem_limit_bytes=56 * 1024 * 1024
        ),
        name="routed",
    )(placed, w_gate, w_up, w_down)
    start = lax.axis_index("sub") * tok_rows
    kept = lax.dynamic_slice(mixed, (0, start, 0), (subs, tok_rows, width))
    return kept.transpose(1, 0, 2).reshape(tok_rows, subs * width)


def solution(mesh):
    return jax.shard_map(
        shards,
        mesh=mesh,
        in_specs=(
            P(("group", "expert", "sub"), None),
            P(("group", "expert", "sub"), None),
            P(("group", "expert", "sub"), None),
            P("expert", ("tensor", "sub"), None),
            P("expert", ("tensor", "sub"), None),
            P("expert", ("tensor", "sub"), None),
        ),
        out_specs=P(("group", "expert", "sub"), "tensor"),
        check_vma=False,
    )
```
